512 devices in a mesh: frag: 2 (over y), band: 128 (over z, x), slab: 2 (over core).
Axes of the slice: x: 8, y: 2, z: 16, core: 2. Of those that a mesh axis runs over, the one named last changes fastest.
The devices are a block of a 8x8x16 slice.
Arguments:
- wavefunctions: bfloat16 [2048, 16384], P('band', ('frag', 'slab')), parts along dimension 1, may hold values from -6 to 6
- eigvec: bfloat16 [2048, 4096], P(None, ('frag', 'band', 'slab')), parts along dimension 1, may hold values from -1 to 1, as said below
- occupation: float32 [4096], P('frag'), parts along dimension 0, may hold values from 0.1 to 2
Outputs:
- rotated: float32 [2048, 16384], P('band', ('frag', 'slab')), parts along dimension 1
- density: float32 [16384], P(('frag', 'slab')), parts along dimension 0
The draws below stay inside these ranges and needn't reach their ends.
There are 2 independent parts, one for each index of `frag`. The reference program is written for one: setup_inputs(seed, part) draws one part's arguments, and reference() takes and returns one part's arrays. A program takes and returns all parts, laid end to end along the dimension named above; each array names one. Nothing has to cross between parts.
Inputs may be any that keep to these rules, and one draw needn't show every extreme that they name: eigvec is an orthogonal matrix rounded to bfloat16.
All inputs are finite; a program needn't handle non-finite values.
Results may differ from the reference program's by a relative error of at most 0.0003.
Values may be sent and summed in bfloat16 or wider, within the bound.
No kernel may reach another device: no remote copies, remote signals or barrier semaphores. Data moves between devices by JAX's collectives and lax.ppermute only.
A program may use at most 64 MiB of HBM per device.

```python
import math
import jax
import jax.numpy as jnp

NB = 2048
NPTS = 8192


def draw_eigvec(key, part):
    sample = jax.random.normal(jax.random.fold_in(key, 7), (NB, NB), jnp.float32)
    basis, upper = jnp.linalg.qr(sample)
    signs = jnp.where(jnp.diagonal(upper) < 0, -1.0, 1.0).astype(jnp.float32)
    return (basis * signs[None, :]).astype(jnp.bfloat16)


def level_of(rng, shape, pieces, low, largest):
    loudness = 1.0
    for dim, shards_of in pieces:
        draws = jax.random.uniform(jax.random.fold_in(jax.random.fold_in(rng, 6), dim), (shards_of,), jnp.float32, low / len(pieces), largest / len(pieces))
        loudness = loudness * jnp.repeat(jnp.exp(draws), shape[dim] // shards_of).reshape((-1,) + (1,) * (len(shape) - 1 - dim))
    return loudness


def normal_values(rng, dims, deviation, limit, cuts=(), held_as=jnp.bfloat16):
    values = deviation * jax.random.normal(rng, dims, jnp.float32)
    if cuts:
        values = values * level_of(rng, dims, cuts, -0.22, 0.18)
    return jnp.clip(values, -limit, limit).astype(held_as)


def setup_inputs(seed: int = 0, part: int = 0) -> dict:
    arg_keys = jax.random.split(jax.random.key(seed), 4)
    part_keys = jax.random.split(jax.random.fold_in(arg_keys[3], part), 4)
    return {
        "wavefunctions": normal_values(part_keys[0], (NB, NPTS), 1.0, 6.0, ((0, 128), (1, 2))),
        "eigvec": draw_eigvec(jax.random.fold_in(jax.random.fold_in(arg_keys[3], part), 71), part),
        "occupation": jnp.clip(jnp.exp(jax.random.uniform(part_keys[2], (NB,), jnp.float32, math.log(0.1), math.log(2.0))), 0.1, 2.0),
    }


def reference(wavefunctions, eigvec, occupation):
    rotated = jnp.dot(eigvec.T.astype(jnp.float32), wavefunctions.astype(jnp.float32), preferred_element_type=jnp.float32)
    weighted = occupation[:, None] * rotated * rotated
    density = jnp.sum(weighted, axis=0) / jnp.float32(NB)
    return (rotated, density)
```

```python
import jax
import jax.numpy as jnp
from jax import lax
from jax.sharding import Mesh
from jax.sharding import PartitionSpec as P

Z = ("zh", "zl")
BAND = ("zh", "zl", "x")


def gathered(array, axis):
    peers = lax.axis_size(axis)
    copies = jnp.broadcast_to(array[None], (peers, *array.shape))
    return lax.all_to_all(copies, axis, 0, 0, tiled=True)


def local(wavefunctions, eigvec, occupation):
    zs, zh, zl, xs, cores = (lax.axis_size(a) for a in (Z, "zh", "zl", "x", "slab"))
    bands, cols = eigvec.shape
    own = wavefunctions.shape[0]
    points = wavefunctions.shape[1] // zs
    pair = xs // zl
    run = zs * own
    quarters = eigvec.T.reshape(cols, zs, xs, own).transpose(2, 0, 1, 3)
    quarters = quarters.reshape(zl, pair, cols, run).transpose(0, 2, 1, 3)
    quarters = quarters.reshape(1, zl, -1, points)
    quarters = jnp.broadcast_to(quarters, (zh, *quarters.shape[1:])).reshape(zs, -1, points)
    blocks = wavefunctions.reshape(own, zs, points).transpose(1, 0, 2)
    met = lax.all_to_all(jnp.concatenate([blocks, quarters], 1), Z, 0, 0, tiled=True)
    old = gathered(met[:, :own].reshape(run, points), "x").reshape(zl, pair, run, points)
    mine = lax.all_gather(met[:, own:].reshape(zs * cols * pair, run), "zl")
    other = lax.ppermute(mine, "slab", [(k, (k + 1) % cores) for k in range(cores)])
    first = lax.axis_index("slab") == 0
    panels = jnp.stack([jnp.where(first, mine, other), jnp.where(first, other, mine)])
    columns = panels.reshape(cores, zl, zs, cols, pair, run).transpose(2, 0, 3, 1, 4, 5)
    columns = columns.reshape(run, bands)
    new = lax.dot_general(
        columns, old.reshape(bands, points), (((1,), (0,)), ((), ())), preferred_element_type=jnp.float32
    )
    weights = lax.dynamic_index_in_dim(occupation.reshape(zs, xs, own), lax.axis_index("x"), 1, False)
    partial = jnp.sum(weights.reshape(run, 1) * new * new, axis=0)
    density = jnp.sum(gathered(partial[None], "x"), axis=0) / jnp.float32(bands)
    sent = jnp.concatenate(
        [new.reshape(zs, own * points), jnp.broadcast_to(density, (zs, points))], axis=1
    )
    got = lax.all_to_all(sent[:, None], Z, 0, 0, tiled=True).reshape(zs, own + 1, points)
    rotated = got[:, :own].transpose(1, 0, 2).reshape(own, zs * points)
    return rotated, got[:, own].reshape(zs * points)


def solution(mesh):
    torus = Mesh(
        mesh.devices.reshape(mesh.shape["frag"], 4, 4, 8, mesh.shape["slab"]),
        ("frag", "zh", "zl", "x", "slab"),
    )
    in_specs = (P(BAND, ("frag", "slab")), P(None, ("frag", *BAND, "slab")), P("frag"))
    out_specs = (P(BAND, ("frag", "slab")), P(("frag", "slab")))
    return jax.shard_map(local, mesh=torus, in_specs=in_specs, out_specs=out_specs, check_vma=False)
```

```python
import jax
import jax.numpy as jnp
from jax import lax
from jax.sharding import Mesh
from jax.sharding import PartitionSpec as P

Z = ("zh", "zl")
BAND = ("zh", "zl", "x")


def gathered(array, axis):
    peers = lax.axis_size(axis)
    copies = jnp.broadcast_to(array[None], (peers, *array.shape))
    return lax.all_to_all(copies, axis, 0, 0, tiled=True)


def exponent(largest):
    return jnp.clip(jnp.floor(jnp.log2(jnp.maximum(largest, 1e-37))), -120.0, 120.0)


def local(wavefunctions, eigvec, occupation):
    zs, zh, zl, xs, cores = (lax.axis_size(a) for a in (Z, "zh", "zl", "x", "slab"))
    bands, cols = eigvec.shape
    own = wavefunctions.shape[0]
    points = wavefunctions.shape[1] // zs
    pair = xs // zl
    run = zs * own
    quarters = eigvec.T.reshape(cols, zs, xs, own).transpose(2, 0, 1, 3)
    quarters = quarters.reshape(zl, pair, cols, run).transpose(0, 2, 1, 3)
    quarters = quarters.reshape(1, zl, -1, points)
    quarters = jnp.broadcast_to(quarters, (zh, *quarters.shape[1:])).reshape(zs, -1, points)
    blocks = wavefunctions.reshape(own, zs, points).transpose(1, 0, 2)
    met = lax.all_to_all(jnp.concatenate([blocks, quarters], 1), Z, 0, 0, tiled=True)
    old = gathered(met[:, :own].reshape(run, points), "x").reshape(zl, pair, run, points)
    mine = lax.all_gather(met[:, own:].reshape(zs * cols * pair, run), "zl")
    other = lax.ppermute(mine, "slab", [(k, (k + 1) % cores) for k in range(cores)])
    first = lax.axis_index("slab") == 0
    panels = jnp.stack([jnp.where(first, mine, other), jnp.where(first, other, mine)])
    columns = panels.reshape(cores, zl, zs, cols, pair, run).transpose(2, 0, 3, 1, 4, 5)
    columns = columns.reshape(run, bands)
    new = lax.dot_general(
        columns, old.reshape(bands, points), (((1,), (0,)), ((), ())), preferred_element_type=jnp.float32
    )
    weights = lax.dynamic_index_in_dim(occupation.reshape(zs, xs, own), lax.axis_index("x"), 1, False)
    partial = jnp.sum(weights.reshape(run, 1) * new * new, axis=0)
    largest = jnp.max(jnp.abs(new), axis=0)
    told = jnp.concatenate([partial, largest]).reshape(1, -1)
    heard = gathered(told, "x").reshape(xs, 2, 2, points // 2)
    power = exponent(largest)
    sent = (new.reshape(zs, own, points) * jnp.exp2(-power)).astype(jnp.float16)
    sent = sent.reshape(zs, own, 2, points // 2).transpose(0, 2, 1, 3).reshape(zs, 2 * own, points // 2)
    density = jnp.sum(heard[:, 0], axis=0) / jnp.float32(bands)
    level = exponent(jnp.max(heard[:, 1], axis=0))
    scaled = (density * jnp.exp2(-level)) * jnp.exp2(-level)
    high = lax.reduce_precision(scaled, 5, 10)
    extra = jnp.concatenate([high, (scaled - high) * 2048.0, power.reshape(2, -1), level]).astype(jnp.float16)
    extra = jnp.broadcast_to(extra[None], (zs, *extra.shape))
    got = lax.all_to_all(jnp.concatenate([sent, extra], 1), Z, 0, 0, tiled=True).astype(jnp.float32)
    extra = got[:, 2 * own :].reshape(zs, 4, 2, points // 2)
    rotated = got[:, : 2 * own].reshape(zs, 2, own, points // 2) * jnp.exp2(extra[:, 2])[:, :, None]
    rotated = rotated.transpose(2, 0, 1, 3).reshape(own, zs * points)
    level = jnp.exp2(extra[:, 3])
    density = ((extra[:, 0] + extra[:, 1] * (1.0 / 2048.0)) * level) * level
    return rotated, density.reshape(zs * points)


def solution(mesh):
    torus = Mesh(
        mesh.devices.reshape(mesh.shape["frag"], 4, 4, 8, mesh.shape["slab"]),
        ("frag", "zh", "zl", "x", "slab"),
    )
    in_specs = (P(BAND, ("frag", "slab")), P(None, ("frag", *BAND, "slab")), P("frag"))
    out_specs = (P(BAND, ("frag", "slab")), P(("frag", "slab")))
    return jax.shard_map(local, mesh=torus, in_specs=in_specs, out_specs=out_specs, check_vma=False)
```

```python
import jax
import jax.numpy as jnp
from jax import lax
from jax.sharding import Mesh
from jax.sharding import PartitionSpec as P

Z = ("zh", "zl")
BAND = ("zh", "zl", "x")


def gathered(array, axis):
    peers = lax.axis_size(axis)
    copies = jnp.broadcast_to(array[None], (peers, *array.shape))
    return lax.all_to_all(copies, axis, 0, 0, tiled=True)


def exponent(largest):
    return jnp.clip(jnp.floor(jnp.log2(jnp.maximum(largest, 1e-37))), -120.0, 120.0)


def steps(wavefunctions, eigvec, occupation):
    zs, zh, zl, xs, cores = (lax.axis_size(a) for a in (Z, "zh", "zl", "x", "slab"))
    bands, cols = eigvec.shape
    own = wavefunctions.shape[0]
    points = wavefunctions.shape[1] // zs
    pair = xs // zl
    run = zs * own
    quarters = eigvec.T.reshape(cols, zs, xs, own).transpose(2, 0, 1, 3)
    quarters = quarters.reshape(1, zl, -1, points)
    quarters = jnp.broadcast_to(quarters, (zh, *quarters.shape[1:])).reshape(zs, -1, points)
    blocks = wavefunctions.reshape(own, zs, points).transpose(1, 0, 2)
    met = lax.all_to_all(jnp.concatenate([blocks, quarters], 1), Z, 0, 0, tiled=True)
    old = gathered(met[:, :own].reshape(run, points), "x").reshape(zl, pair, run, points)
    mine = lax.all_gather(met[:, own:].reshape(zs * cols * pair, run), "zl")
    other = lax.ppermute(mine, "slab", [(k, (k + 1) % cores) for k in range(cores)])
    first = lax.axis_index("slab") == 0
    chosen = [jnp.where(first, mine, other), jnp.where(first, other, mine)]
    chosen = [c.reshape(zl, zs, pair, cols, run) for c in chosen]
    columns = jnp.concatenate(
        [jnp.stack([c[k, :, p] for c in chosen], 1).reshape(run, run) for k in range(zl) for p in range(pair)], axis=1
    )
    new = lax.dot_general(
        columns, old.reshape(bands, points), (((1,), (0,)), ((), ())), preferred_element_type=jnp.float32
    )
    weights = lax.dynamic_index_in_dim(occupation.reshape(zs, xs, own), lax.axis_index("x"), 1, False)
    partial = jnp.sum(weights.reshape(run, 1) * new * new, axis=0)
    largest = jnp.max(jnp.abs(new), axis=0)
    told = jnp.concatenate([partial, largest]).reshape(1, -1)
    heard = gathered(told, "x").reshape(xs, 2, 2, points // 2)
    power = exponent(largest)
    sent = (new.reshape(zs, own, points) * jnp.exp2(-power)).astype(jnp.float16)
    sent = sent.reshape(zs, own, 2, points // 2).transpose(0, 2, 1, 3).reshape(zs, 2 * own, points // 2)
    density = jnp.sum(heard[:, 0], axis=0) / jnp.float32(bands)
    level = exponent(jnp.max(heard[:, 1], axis=0))
    scaled = (density * jnp.exp2(-level)) * jnp.exp2(-level)
    high = lax.reduce_precision(scaled, 5, 10)
    extra = jnp.concatenate([high, (scaled - high) * 2048.0, power.reshape(2, -1), level]).astype(jnp.float16)
    extra = jnp.broadcast_to(extra[None], (zs, *extra.shape))
    got = lax.all_to_all(jnp.concatenate([sent, extra], 1), Z, 0, 0, tiled=True).astype(jnp.float32)
    extra = got[:, 2 * own :].reshape(zs, 4, 2, points // 2)
    rotated = got[:, : 2 * own].reshape(zs, 2, own, points // 2) * jnp.exp2(extra[:, 2])[:, :, None]
    rotated = jnp.concatenate([rotated[k, h] for k in range(zs) for h in range(2)], axis=1)
    level = jnp.exp2(extra[:, 3])
    density = ((extra[:, 0] + extra[:, 1] * (1.0 / 2048.0)) * level) * level
    return rotated, density.reshape(zs * points)


def solution(mesh):
    torus = Mesh(
        mesh.devices.reshape(mesh.shape["frag"], 2, 8, 8, mesh.shape["slab"]),
        ("frag", "zh", "zl", "x", "slab"),
    )
    in_specs = (P(BAND, ("frag", "slab")), P(None, ("frag", *BAND, "slab")), P("frag"))
    out_specs = (P(BAND, ("frag", "slab")), P(("frag", "slab")))
    return jax.shard_map(steps, mesh=torus, in_specs=in_specs, out_specs=out_specs, check_vma=False)
```
